128 devices in a mesh: fsdp: 8 (over x, core), ep: 16 (over z, y).
Axes of the slice: x: 4, y: 4, z: 4, core: 2. Of those that a mesh axis runs over, the one named last changes fastest.
Arguments:
- hidden_rows: bfloat16 [4096, 2, 4096], P('fsdp'), may hold values from -6 to 6
- norm_gain: float32 [4096], replicated, may hold values from 0.1 to 1.9
- route_expert: int32 [4096, 2, 2], P('fsdp'), may hold values from 0 to 3, all different within a row
- route_weight: float32 [4096, 2, 2], P('fsdp'), may hold values from 0.2 to 1
- gate_base: bfloat16 [16, 4096, 384], P('ep'), may hold values from -0.09375 to 0.09375
- up_base: bfloat16 [16, 4096, 384], P('ep'), may hold values from -0.09375 to 0.09375
- down_base: bfloat16 [16, 384, 4096], P('ep'), may hold values from -0.15625 to 0.15625
- tile_values: bfloat16 [4096, 128, 128], P(('fsdp', 'ep')), may hold values from -6 to 6
- tile_scale: float32 [4096], P(('fsdp', 'ep')), may hold values from 0.01 to 0.08
- tile_owner: int32 [4096, 1], P(('fsdp', 'ep')), may hold values from 0 to 15; in each aligned block of 32 rows (0 to 31, 32 to 63, ...) at most 4 rows name the same one
- tile_slot: int32 [4096], P(('fsdp', 'ep')), may hold values from 0 to 287
Outputs:
- layer_out: bfloat16 [4096, 2, 4096], P(('fsdp', 'ep'))
The draws below stay inside these ranges and needn't reach their ends.
Inputs may be any that keep to these rules, and one draw needn't show every extreme that they name: `tile_owner`: among the 32 tiles of one trainer device no owner is named more than 4 times. `route_expert`: each row and step names 2 different experts.
All inputs are finite; a program needn't handle non-finite values.
Results may differ from the reference program's by a relative error of at most 0.022.
Values may be sent and summed in bfloat16 or wider, within the bound.
No kernel may reach another device: no remote copies, remote signals or barrier semaphores. Data moves between devices by JAX's collectives and lax.ppermute only.
A program may use at most 256 MiB of HBM per device.

```python
import math
import jax
import jax.numpy as jnp
import numpy as np
from jax import lax

D = 4096
FF = 1536
TB = 128
TSPLIT = 4
TOP = 2
STEPS = 2
TILE_DEV = 32
CAP = 4
HID = 384
EXPERTS = 4
TILES = 4096
SLOTS = 288
ROWS_ALL = 4096
N_EP = 16


def set_ends(result, rng, low, high):
    place = [jax.random.randint(jax.random.fold_in(rng, axis), (), 0, length) for axis, length in enumerate(result.shape)]
    longest = result.shape.index(max(result.shape))
    neighbour = place[:longest] + [(place[longest] + 1) % result.shape[longest]] + place[longest + 1:]
    return result.at[tuple(place)].set(low).at[tuple(neighbour)].set(high)


def levels(own_key, dims, shards, low, top_value):
    def one(dim, parts):
        heights = jax.random.uniform(jax.random.fold_in(jax.random.fold_in(own_key, 6), dim), (parts,), jnp.float32, low / len(shards), top_value / len(shards))
        return jnp.repeat(jnp.exp(heights), dims[dim] // parts).reshape((-1,) + (1,) * (len(dims) - dim - 1))

    level = one(*shards[0])
    for cut in shards[1:]:
        level = level * one(*cut)
    return level


def different_ones(stream_key, rows, number_of, top, lift):
    order = jax.random.permutation(jax.random.fold_in(stream_key, 1), number_of)
    favour = order
    for power in range(3):
        favour = favour * favour // number_of
    favour = favour * lift // number_of
    tickets = jax.random.randint(jax.random.fold_in(stream_key, 2), (rows, number_of), 0, 4096) + favour
    fixed_rows = jax.random.permutation(jax.random.fold_in(stream_key, 3), rows)[jnp.arange(number_of) % rows]
    tickets = jnp.where(jnp.arange(rows)[:, None] == fixed_rows[None, :], 1 << 14, tickets)
    score = tickets * number_of + jnp.arange(number_of)
    return lax.top_k(score.astype(jnp.int32), top)[1].astype(jnp.int32)


def shared_out(own_key, own, number, rows, number_of, top, limit, skew):
    sequence = jax.random.permutation(own_key, number_of)
    packed, common = shares(number_of, rows * top, limit, skew, True), shares(number_of, rows * top, limit, skew, False)
    places = jnp.arange(number_of)

    def named(tallies, rotation):
        used = int((tallies > 0).sum())
        fixed = max(1, used // 4)
        shifted = fixed + (places - fixed + rotation * (used - fixed)) % max(1, number_of - fixed)
        return jnp.zeros((number_of,), jnp.int32).at[sequence[jnp.where(places < fixed, places, shifted)]].set(jnp.asarray(tallies, jnp.int32))

    tallies = jnp.where(number % 4 == 0, named(packed, number // 4), named(common, number - number // 4 - 1))
    mixed = jax.random.permutation(jax.random.fold_in(own, 3), number_of)
    source_of, sink = mixed[0:number_of // 2 * 2:2], mixed[1:number_of // 2 * 2:2]
    margin = jnp.minimum(tallies[source_of] - 1, limit - tallies[sink]) // 2
    margin = jnp.where((source_of == sequence[0]) | (sink == sequence[0]) | (tallies[sink] == 0), 0, jnp.maximum(margin, 0))
    shifted = jax.random.randint(jax.random.fold_in(own, 4), (number_of // 2,), 0, 1 << 20) % (margin + 1)
    tallies = tallies.at[source_of].add(-shifted).at[sink].add(shifted)
    members = jnp.searchsorted(jnp.cumsum(tallies), jnp.arange(rows * top), side="right").astype(jnp.int32)
    grid = members.reshape(top, rows).T
    grid = grid[jax.random.permutation(jax.random.fold_in(own, 1), rows)]
    rotation = jax.random.randint(jax.random.fold_in(own, 2), (rows, 1), 0, top)
    return jnp.take_along_axis(grid, (jnp.arange(top)[None, :] + rotation) % top, axis=1)


def shares(count, total, reach, skew, full):
    loads = [(1 << 20) // math.isqrt(rank ** skew) + 1 for rank in range(1, count + 1)]
    largest = reach if full else min(reach, max(-(-total // count), total * loads[0] // sum(loads)))
    least = 1 if total - largest >= count - 1 else 0
    given, rest = [largest] + [least] * (count - 1), total - largest - least * (count - 1)
    while rest > 0:
        free = [i for i in range(1, count) if given[i] < largest] or [i for i in range(1, count) if given[i] < reach]
        pool, budget = sum([loads[i] for i in free]), rest
        for i in free:
            more = min(reach - given[i], max(1, budget * loads[i] // pool), rest)
            given[i] = given[i] + more
            rest = rest - more
    return np.array(given)


def bell_draw(key, dims, width, most, cuts=(), held_as=jnp.bfloat16):
    entries = width * jax.random.normal(key, dims, jnp.float32)
    if cuts:
        entries = entries * levels(key, dims, cuts, -0.22, 0.18)
    return jnp.clip(entries, -most, most).astype(held_as)


def setup_inputs(seed: int = 0) -> dict:
    key_list = jax.random.split(jax.random.key(seed), 12)
    hidden_rows = bell_draw(key_list[0], (ROWS_ALL, STEPS, D), 1.0, 6.0, ((0, 8),))
    norm_gain = jnp.clip(1.0 + 0.18 * jax.random.normal(key_list[1], (D,), jnp.float32), 0.1, 1.9)
    route_expert = different_ones(key_list[2], ROWS_ALL * STEPS, EXPERTS, TOP, 4096).reshape((ROWS_ALL, STEPS, TOP))
    route_weight = jnp.clip(0.2 + 0.8 * jax.random.uniform(key_list[3], (ROWS_ALL, STEPS, TOP), jnp.float32) ** levels(key_list[3], (ROWS_ALL, STEPS, TOP), ((0, 8),), -0.2, 0.2), 0.2, 1.0)
    gate_base = bell_draw(key_list[4], (N_EP, D, HID), D ** -0.5, 0.09375, ((0, 16),))
    up_base = bell_draw(key_list[5], (N_EP, D, HID), D ** -0.5, 0.09375, ((0, 16),))
    down_base = bell_draw(key_list[6], (N_EP, HID, D), FF ** -0.5, 0.15625, ((0, 16),))
    tile_values = bell_draw(key_list[7], (TILES, TB, TB), 1.0, 6.0, ((0, 128),))
    tile_scale = jnp.clip(jnp.exp(math.log(0.08) - 2.0794415 * jax.random.uniform(key_list[8], (TILES,), jnp.float32) ** levels(key_list[8], (TILES,), ((0, 128),), -0.2, 0.2)), 0.01, 0.08)
    tile_owner_keys = jax.random.split(jax.random.fold_in(key_list[9], 1), TILES // TILE_DEV)
    tile_owner_turns = jax.random.permutation(jax.random.fold_in(key_list[9], 3), TILES // TILE_DEV)
    tile_owner = jax.vmap(lambda own, number: shared_out(jax.random.fold_in(key_list[9], 2), own, number, TILE_DEV, N_EP, 1, CAP, 2))(tile_owner_keys, tile_owner_turns).reshape((TILES, 1))
    tile_slot = set_ends(jax.random.randint(key_list[10], (TILES,), 0, SLOTS), jax.random.fold_in(key_list[10], 1), 0, SLOTS - 1).astype(jnp.int32)
    return dict(hidden_rows=hidden_rows, norm_gain=norm_gain, route_expert=route_expert, route_weight=route_weight, gate_base=gate_base, up_base=up_base, down_base=down_base, tile_values=tile_values, tile_scale=tile_scale, tile_owner=tile_owner, tile_slot=tile_slot)


EPSILON = 1e-06

def normalize(hidden_rows, norm_gain):
    values = hidden_rows.astype(jnp.float32)
    scaled = values * lax.rsqrt(lax.optimization_barrier(jnp.mean(values * values, axis=-1, keepdims=True)) + EPSILON)
    return (scaled * norm_gain.astype(jnp.float32)).astype(jnp.bfloat16)

def unfold_delta(delta):
    row_blocks = D // TB
    col_blocks = HID // TB
    third = row_blocks * col_blocks
    gate_part = delta[:third].reshape(row_blocks, col_blocks, TB, TB).transpose(0, 2, 1, 3).reshape(D, HID)
    up_part = delta[third:2 * third].reshape(row_blocks, col_blocks, TB, TB).transpose(0, 2, 1, 3).reshape(D, HID)
    down_part = delta[2 * third:].reshape(col_blocks, row_blocks, TB, TB).transpose(0, 2, 1, 3).reshape(HID, D)
    return (gate_part, up_part, down_part)

def refreshed(gate_old, up_old, down_old, delta):
    gate_part, up_part, down_part = unfold_delta(delta)
    gate_new = (gate_old.astype(jnp.float32) + gate_part).astype(jnp.bfloat16)
    up_new = (up_old.astype(jnp.float32) + up_part).astype(jnp.bfloat16)
    down_new = (down_old.astype(jnp.float32) + down_part).astype(jnp.bfloat16)
    return (gate_new, up_new, down_new)

def expert_out(inputs, combine, gate_new, up_new, down_new):
    gate = jnp.dot(inputs, gate_new, preferred_element_type=jnp.float32)
    upward = jnp.dot(inputs, up_new, preferred_element_type=jnp.float32)
    hidden = (jax.nn.silu(gate) * upward * combine).astype(jnp.bfloat16)
    return jnp.dot(hidden, down_new, preferred_element_type=jnp.float32)

def reference(hidden_rows, norm_gain, route_expert, route_weight, gate_base, up_base, down_base, tile_values, tile_scale, tile_owner, tile_slot):
    owner_count = gate_base.shape[0]
    scaled_tiles = tile_values.astype(jnp.float32) * tile_scale[:, None, None]
    deltas = jnp.zeros((owner_count, SLOTS, TB, TB), jnp.float32).at[tile_owner[:, 0], tile_slot].add(scaled_tiles)
    normed = normalize(hidden_rows, norm_gain)
    inputs = normed.reshape(-1, D)

    def add_owner(total, owner):
        gate_new, up_new, down_new = refreshed(gate_base[owner], up_base[owner], down_base[owner], deltas[owner])
        expert = owner // TSPLIT
        combine = lax.optimization_barrier(jnp.sum(jnp.where(route_expert == expert, route_weight, 0.0), axis=-1)).reshape(-1, 1)
        return (total + expert_out(inputs, combine, gate_new, up_new, down_new), owner)
    total, unused = lax.scan(add_owner, jnp.zeros((inputs.shape[0], D), jnp.float32), jnp.arange(owner_count, dtype=jnp.int32))
    return total.reshape(hidden_rows.shape).astype(jnp.bfloat16)
```

```python
import jax
import jax.numpy as jnp
from jax import lax
from jax.experimental import pallas as pl
from jax.experimental.pallas import tpu as pltpu
from jax.sharding import Mesh, PartitionSpec as P

D = 4096
TB = 128
TSPLIT = 4
CAP = 4
HID = 384
OWNERS = 16
SLOTS = 288
META = 16
EPSILON = 1e-06
BF = jnp.bfloat16
F32 = jnp.float32
EP = ("z", "y")


def pack_kernel(owner, slot, scale, tiles, send, counts, meta, meta_low, sems, meta_sem):
    held = tiles.shape[0]
    rows = CAP * TB

    def clear(o, _):
        counts[o] = 0
        return _

    lax.fori_loop(0, OWNERS, clear, 0)
    meta[...] = jnp.zeros_like(meta)

    def copy(i, o, r):
        return pltpu.make_async_copy(tiles.at[i], send.at[o, pl.ds(r * TB, TB), :], sems.at[i])

    def place(i, _):
        o = owner[i]
        r = counts[o]
        counts[o] = r + 1
        copy(i, o, r).start()
        code = slot[i] + 1
        value = jnp.full((1, TB), scale[i], F32)
        high = value.astype(BF).astype(F32)
        meta[o, pl.ds(r * 4, 1), :] = jnp.full((1, TB), (code // 16).astype(F32), F32)
        meta[o, pl.ds(r * 4 + 1, 1), :] = jnp.full((1, TB), (code % 16).astype(F32), F32)
        meta[o, pl.ds(r * 4 + 2, 1), :] = high
        meta[o, pl.ds(r * 4 + 3, 1), :] = value - high
        return _

    lax.fori_loop(0, held, place, 0)
    meta_low[...] = meta[...].astype(BF)
    meta_copy = pltpu.make_async_copy(meta_low, send.at[:, pl.ds(rows, META), :], meta_sem)
    meta_copy.start()

    def finish(i, _):
        copy(i, 0, 0).wait()
        return _

    lax.fori_loop(0, held, finish, 0)
    meta_copy.wait()


def pack(owner, slot, scale, tiles):
    smem = pl.BlockSpec(memory_space=pltpu.SMEM)
    held = tiles.shape[0]
    return pl.pallas_call(
        pack_kernel,
        out_shape=jax.ShapeDtypeStruct((OWNERS, CAP * TB + META, TB), BF),
        in_specs=[smem, smem, smem, pl.BlockSpec(memory_space=pltpu.VMEM)],
        out_specs=pl.BlockSpec(memory_space=pl.ANY),
        scratch_shapes=[
            pltpu.SMEM((OWNERS,), jnp.int32),
            pltpu.VMEM((OWNERS, META, TB), F32),
            pltpu.VMEM((OWNERS, META, TB), BF),
            pltpu.SemaphoreType.DMA((held,)),
            pltpu.SemaphoreType.DMA,
        ],
        name="pack",
    )(owner, slot, scale, tiles)


GROUPS_STEP = 8


def refresh_kernel(slots, scales, got, gate, up, down, gate_out, up_out, down_out, delta):
    step = pl.program_id(0)
    steps = pl.num_programs(0)

    @pl.when(step == 0)
    def _():
        def clear(s, _):
            delta[s] = jnp.zeros((TB, TB), F32)
            return _

        lax.fori_loop(0, SLOTS + 1, clear, 0, unroll=4)

    def add(g, _):
        for r in range(CAP):
            place = (step * GROUPS_STEP + g) * CAP + r
            s = slots[place]
            delta[s] += got[g, pl.ds(r * TB, TB), :].astype(F32) * scales[place]
        return _

    lax.fori_loop(0, GROUPS_STEP, add, 0)

    @pl.when(step == steps - 1)
    def _():
        cols = HID // TB

        def wide(b, _):
            for c in range(cols):
                part = (pl.ds(b * TB, TB), pl.ds(c * TB, TB))
                gate_out[part] = (gate[part].astype(F32) + delta[b * cols + c]).astype(BF)
                up_out[part] = (up[part].astype(F32) + delta[SLOTS // 3 + b * cols + c]).astype(BF)
                tall = (pl.ds(c * TB, TB), pl.ds(b * TB, TB))
                down_out[tall] = (down[tall].astype(F32) + delta[2 * (SLOTS // 3) + c * (D // TB) + b]).astype(BF)
            return _

        lax.fori_loop(0, D // TB, wide, 0)


def refresh(slots, scales, got, gate, up, down):
    whole = lambda shape: pl.BlockSpec(shape, lambda i, *_: (0,) * len(shape), pipeline_mode=pl.Buffered(1))
    groups = got.shape[0]
    wide, tall = (D, HID), (HID, D)
    return pl.pallas_call(
        refresh_kernel,
        out_shape=[jax.ShapeDtypeStruct(s, BF) for s in (wide, wide, tall)],
        grid_spec=pltpu.PrefetchScalarGridSpec(
            num_scalar_prefetch=2,
            grid=(groups // GROUPS_STEP,),
            in_specs=[
                pl.BlockSpec((GROUPS_STEP,) + got.shape[1:], lambda i, *_: (i, 0, 0)),
                whole(wide),
                whole(wide),
                whole(tall),
            ],
            out_specs=[whole(wide), whole(wide), whole(tall)],
            scratch_shapes=[pltpu.VMEM((SLOTS + 1, TB, TB), F32)],
        ),
        compiler_params=pltpu.CompilerParams(dimension_semantics=("arbitrary",), vmem_limit_bytes=60 << 20),
        name="refresh",
    )(slots, scales, got, gate, up, down)


ROWS_STEP = 256


def expert_kernel(normed, combine, gate, up, down, out):
    block = normed[...]
    g = jnp.dot(block, gate[...], preferred_element_type=F32)
    u = jnp.dot(block, up[...], preferred_element_type=F32)
    hidden = (jax.nn.silu(g) * u * combine[...]).astype(BF)
    out[...] = jnp.dot(hidden, down[...], preferred_element_type=F32).astype(BF)


def expert(normed, combine, gate, up, down):
    whole = lambda shape: pl.BlockSpec(shape, lambda i: (0,) * len(shape), pipeline_mode=pl.Buffered(1))
    rows = normed.shape[0]
    return pl.pallas_call(
        expert_kernel,
        out_shape=jax.ShapeDtypeStruct((rows, D), BF),
        grid=(rows // ROWS_STEP,),
        in_specs=[
            pl.BlockSpec((ROWS_STEP, D), lambda i: (i, 0)),
            pl.BlockSpec((ROWS_STEP, 1), lambda i: (i, 0)),
            whole((D, HID)),
            whole((D, HID)),
            whole((HID, D)),
        ],
        out_specs=pl.BlockSpec((ROWS_STEP, D), lambda i: (i, 0)),
        compiler_params=pltpu.CompilerParams(dimension_semantics=("arbitrary",), vmem_limit_bytes=60 << 20),
        name="expert",
    )(normed, combine, gate, up, down)


def normalize(hidden_rows, norm_gain):
    values = hidden_rows.astype(F32)
    scaled = values * lax.rsqrt(jnp.mean(values * values, axis=-1, keepdims=True) + EPSILON)
    return (scaled * norm_gain).astype(BF)


def unpack_meta(meta):
    fields = meta.astype(F32).reshape(-1, CAP, 4)
    code = (fields[..., 0] * 16.0 + fields[..., 1]).astype(jnp.int32)
    slots = jnp.where(code > 0, code - 1, SLOTS)
    scales = fields[..., 2] + fields[..., 3]
    return slots.reshape(-1), scales.reshape(-1)


def body(
    hidden_rows,
    norm_gain,
    route_expert,
    route_weight,
    gate_base,
    up_base,
    down_base,
    tile_values,
    tile_scale,
    tile_owner,
    tile_slot,
):
    send = pack(tile_owner[:, 0], tile_slot, tile_scale, tile_values)
    got = lax.all_to_all(send, EP, split_axis=0, concat_axis=0, tiled=True)
    got = lax.all_gather(got, ("x", "c"), axis=0, tiled=True)
    slots, scales = unpack_meta(got[:, CAP * TB :, 0])
    gate_new, up_new, down_new = refresh(slots, scales, got, gate_base[0], up_base[0], down_base[0])
    normed = normalize(hidden_rows, norm_gain).reshape(-1, D)
    own = lax.axis_index("z")
    combine = jnp.sum(jnp.where(route_expert == own, route_weight, 0.0), axis=-1).reshape(-1, 1)
    part = expert(normed, combine, gate_new, up_new, down_new)
    out = lax.psum_scatter(part, EP, scatter_dimension=0, tiled=True)
    return out.reshape(-1, hidden_rows.shape[1], D)


def solution(mesh):
    fine = Mesh(mesh.devices.reshape(4, 2, 4, 4), ("x", "c", "z", "y"))
    rows = ("x", "c")
    every = ("x", "c", "z", "y")
    return jax.shard_map(
        body,
        mesh=fine,
        in_specs=(
            P(rows, None, None),
            P(),
            P(rows, None, None),
            P(rows, None, None),
            P(EP, None, None),
            P(EP, None, None),
            P(EP, None, None),
            P(every, None, None),
            P(every),
            P(every, None),
            P(every),
        ),
        out_specs=P(every, None, None),
        check_vma=False,
    )
```

```python
import jax
import jax.numpy as jnp
from jax import lax
from jax.experimental import pallas as pl
from jax.experimental.pallas import tpu as pltpu
from jax.sharding import Mesh, PartitionSpec as P

D = 4096
TB = 128
TSPLIT = 4
CAP = 4
HID = 384
OWNERS = 16
SLOTS = 288
META = 16
EPSILON = 1e-06
BF = jnp.bfloat16
F32 = jnp.float32
EP = ("z", "y")


def pack_kernel(owner, slot, scale, tiles, send, counts, meta, meta_low, sems, meta_sem):
    held = tiles.shape[0]
    rows = CAP * TB

    def clear(o, _):
        counts[o] = 0
        return _

    lax.fori_loop(0, OWNERS, clear, 0)
    meta[...] = jnp.zeros_like(meta)

    def copy(i, o, r):
        return pltpu.make_async_copy(tiles.at[i], send.at[o, pl.ds(r * TB, TB), :], sems.at[i])

    def place(i, _):
        o = owner[i]
        r = counts[o]
        counts[o] = r + 1
        copy(i, o, r).start()
        code = slot[i] + 1
        value = jnp.full((1, TB), scale[i], F32)
        high = value.astype(BF).astype(F32)
        meta[o, pl.ds(r * 4, 1), :] = jnp.full((1, TB), (code // 16).astype(F32), F32)
        meta[o, pl.ds(r * 4 + 1, 1), :] = jnp.full((1, TB), (code % 16).astype(F32), F32)
        meta[o, pl.ds(r * 4 + 2, 1), :] = high
        meta[o, pl.ds(r * 4 + 3, 1), :] = value - high
        return _

    lax.fori_loop(0, held, place, 0)
    meta_low[...] = meta[...].astype(BF)
    meta_copy = pltpu.make_async_copy(meta_low, send.at[:, pl.ds(rows, META), :], meta_sem)
    meta_copy.start()

    def finish(i, _):
        copy(i, 0, 0).wait()
        return _

    lax.fori_loop(0, held, finish, 0)
    meta_copy.wait()


def pack(owner, slot, scale, tiles):
    smem = pl.BlockSpec(memory_space=pltpu.SMEM)
    held = tiles.shape[0]
    return pl.pallas_call(
        pack_kernel,
        out_shape=jax.ShapeDtypeStruct((OWNERS, CAP * TB + META, TB), BF),
        in_specs=[smem, smem, smem, pl.BlockSpec(memory_space=pltpu.VMEM)],
        out_specs=pl.BlockSpec(memory_space=pl.ANY),
        scratch_shapes=[
            pltpu.SMEM((OWNERS,), jnp.int32),
            pltpu.VMEM((OWNERS, META, TB), F32),
            pltpu.VMEM((OWNERS, META, TB), BF),
            pltpu.SemaphoreType.DMA((held,)),
            pltpu.SemaphoreType.DMA,
        ],
        name="pack",
    )(owner, slot, scale, tiles)


GROUPS_STEP = 8


def refresh_kernel(slots, scales, got, gate, up, down, gate_out, up_out, down_out, delta):
    step = pl.program_id(0)
    steps = pl.num_programs(0)

    @pl.when(step == 0)
    def _():
        def clear(s, _):
            delta[s] = jnp.zeros((TB, TB), F32)
            return _

        lax.fori_loop(0, SLOTS + 1, clear, 0, unroll=4)

    def add(g, _):
        for r in range(CAP):
            place = (step * GROUPS_STEP + g) * CAP + r
            s = slots[place]
            delta[s] += got[g, pl.ds(r * TB, TB), :].astype(F32) * scales[place]
        return _

    lax.fori_loop(0, GROUPS_STEP, add, 0)

    @pl.when(step == steps - 1)
    def _():
        cols = HID // TB

        def wide(b, _):
            for c in range(cols):
                part = (pl.ds(b * TB, TB), pl.ds(c * TB, TB))
                gate_out[part] = (gate[part].astype(F32) + delta[b * cols + c]).astype(BF)
                up_out[part] = (up[part].astype(F32) + delta[SLOTS // 3 + b * cols + c]).astype(BF)
                tall = (pl.ds(c * TB, TB), pl.ds(b * TB, TB))
                down_out[tall] = (down[tall].astype(F32) + delta[2 * (SLOTS // 3) + c * (D // TB) + b]).astype(BF)
            return _

        lax.fori_loop(0, D // TB, wide, 0)


def refresh(slots, scales, got, gate, up, down):
    whole = lambda shape: pl.BlockSpec(shape, lambda i, *_: (0,) * len(shape), pipeline_mode=pl.Buffered(1))
    groups = got.shape[0]
    wide, tall = (D, HID), (HID, D)
    return pl.pallas_call(
        refresh_kernel,
        out_shape=[jax.ShapeDtypeStruct(s, BF) for s in (wide, wide, tall)],
        grid_spec=pltpu.PrefetchScalarGridSpec(
            num_scalar_prefetch=2,
            grid=(groups // GROUPS_STEP,),
            in_specs=[
                pl.BlockSpec((GROUPS_STEP,) + got.shape[1:], lambda i, *_: (i, 0, 0)),
                whole(wide),
                whole(wide),
                whole(tall),
            ],
            out_specs=[whole(wide), whole(wide), whole(tall)],
            scratch_shapes=[pltpu.VMEM((SLOTS + 1, TB, TB), F32)],
        ),
        compiler_params=pltpu.CompilerParams(dimension_semantics=("arbitrary",), vmem_limit_bytes=60 << 20),
        name="refresh",
    )(slots, scales, got, gate, up, down)


PIECE = 16
PIECES = 16


def expert_kernel(starts, normed, combine, gate, up, down, *rest):
    outs, (block, weight, sems) = rest[:-3], rest[-3:]

    def rows(i):
        return pl.ds(pl.multiple_of(starts[i], PIECE), PIECE), pl.ds(i * PIECE, PIECE)

    def copy(i):
        there, here = rows(i)
        return pltpu.make_async_copy(normed.at[there, :], block.at[here, :], sems.at[i])

    for i in range(PIECES):
        copy(i).start()
    for i in range(PIECES):
        there, here = rows(i)
        weight[here, :] = combine[there, :]
    for i in range(PIECES):
        copy(i).wait()
    x = block[...]
    g = jnp.dot(x, gate[...], preferred_element_type=F32)
    u = jnp.dot(x, up[...], preferred_element_type=F32)
    hidden = (jax.nn.silu(g) * u * weight[:, :1]).astype(BF)
    part = jnp.dot(hidden, down[...], preferred_element_type=F32).astype(BF)
    first = 0
    for out in outs:
        out[...] = part[first : first + out.shape[0]]
        first += out.shape[0]


def expert(starts, normed, combine, weights, parts):
    hbm = pl.BlockSpec(memory_space=pl.ANY)
    vmem = pl.BlockSpec(memory_space=pltpu.VMEM)
    rows = PIECE * PIECES
    return pl.pallas_call(
        expert_kernel,
        out_shape=[jax.ShapeDtypeStruct((n, D), BF) for n in parts],
        in_specs=[pl.BlockSpec(memory_space=pltpu.SMEM), hbm, vmem, vmem, vmem, vmem],
        out_specs=[vmem] * len(parts),
        scratch_shapes=[
            pltpu.VMEM((rows, D), BF),
            pltpu.VMEM((rows, TB), F32),
            pltpu.SemaphoreType.DMA((PIECES,)),
        ],
        compiler_params=pltpu.CompilerParams(vmem_limit_bytes=48 << 20),
        name="expert",
    )(starts, normed, combine, *weights)


def shift(value, axis, by):
    n = lax.axis_size(axis)
    return lax.ppermute(value, axis, [(i, (i + by) % n) for i in range(n)])


def total(*terms):
    out = terms[0].astype(F32)
    for term in terms[1:]:
        out = out + term.astype(F32)
    return out.astype(BF)


def rows_of(half, first, second, first_at, second_at, blocks):
    starts = []
    for offset, quarter in blocks:
        for k in range(4):
            a, b = (first_at + offset) % 4, (second_at + k) % 4
            z, y = (b, a) if first == "y" else (a, b)
            starts.append((z * 4 + y) * 64 + half * 32 + quarter * PIECE)
    return jnp.stack(starts).astype(jnp.int32)


def send_part(half, first, second, run):
    at = lax.axis_index(first), lax.axis_index(second)
    plus, minus = run(rows_of(half, first, second, *at, ((2, 0), (1, 1), (2, 1), (3, 0))), (128, 128))
    return shift(plus, first, 1), shift(minus, first, -1)


def sum_part(half, first, second, run, got_plus, got_minus):
    at = lax.axis_index(first), lax.axis_index(second)
    keep_plus, keep_minus, own = run(
        rows_of(half, first, second, *at, ((1, 0), (3, 1), (0, 0), (0, 1))), (64, 64, 128)
    )
    last_plus = shift(total(got_plus[:64], keep_plus), first, 1)
    last_minus = shift(total(got_minus[:64], keep_minus), first, -1)
    sums = []
    for k in range(4):
        at_k = slice(k * PIECE, (k + 1) * PIECE)
        upper = total(own[:64][at_k], got_minus[64:][at_k], last_plus[at_k])
        lower = total(own[64:][at_k], got_plus[64:][at_k], last_minus[at_k])
        sums.append(jnp.concatenate([upper, lower], axis=0))
    return total(sums[0], *(shift(sums[k], second, (1, 2, -1)[k - 1]) for k in (1, 2, 3)))


def normalize(hidden_rows, norm_gain):
    values = hidden_rows.astype(F32)
    scaled = values * lax.rsqrt(jnp.mean(values * values, axis=-1, keepdims=True) + EPSILON)
    return (scaled * norm_gain).astype(BF)


def unpack_meta(meta):
    fields = meta.astype(F32).reshape(-1, CAP, 4)
    code = (fields[..., 0] * 16.0 + fields[..., 1]).astype(jnp.int32)
    slots = jnp.where(code > 0, code - 1, SLOTS)
    scales = fields[..., 2] + fields[..., 3]
    return slots.reshape(-1), scales.reshape(-1)


def body(
    hidden_rows,
    norm_gain,
    route_expert,
    route_weight,
    gate_base,
    up_base,
    down_base,
    tile_values,
    tile_scale,
    tile_owner,
    tile_slot,
):
    send = pack(tile_owner[:, 0], tile_slot, tile_scale, tile_values)
    got = lax.all_to_all(send, EP, split_axis=0, concat_axis=0, tiled=True)
    got = lax.all_gather(got, ("x", "c"), axis=0, tiled=True)
    slots, scales = unpack_meta(got[:, CAP * TB :, 0])
    gate_new, up_new, down_new = refresh(slots, scales, got, gate_base[0], up_base[0], down_base[0])
    normed = normalize(hidden_rows, norm_gain).reshape(-1, D)
    own = lax.axis_index("z")
    combine = jnp.sum(jnp.where(route_expert == own, route_weight, 0.0), axis=-1).reshape(-1, 1)
    combine = jnp.broadcast_to(combine, (combine.shape[0], TB))
    weights = gate_new, up_new, down_new
    run = lambda starts, parts: expert(starts, normed, combine, weights, parts)
    got_a = send_part(0, "y", "z", run)
    got_b = send_part(1, "z", "y", run)
    out_a = sum_part(0, "y", "z", run, *got_a)
    out_b = sum_part(1, "z", "y", run, *got_b)
    return jnp.concatenate([out_a, out_b], axis=0).reshape(-1, hidden_rows.shape[1], D)


def solution(mesh):
    fine = Mesh(mesh.devices.reshape(4, 2, 4, 4), ("x", "c", "z", "y"))
    rows = ("x", "c")
    every = ("x", "c", "z", "y")
    return jax.shard_map(
        body,
        mesh=fine,
        in_specs=(
            P(rows, None, None),
            P(),
            P(rows, None, None),
            P(rows, None, None),
            P(EP, None, None),
            P(EP, None, None),
            P(EP, None, None),
            P(every, None, None),
            P(every),
            P(every, None),
            P(every),
        ),
        out_specs=P(every, None, None),
        check_vma=False,
    )
```

```python
import jax
import jax.numpy as jnp
from jax import lax
from jax.experimental import pallas as pl
from jax.experimental.pallas import tpu as pltpu
from jax.sharding import Mesh, PartitionSpec as P

D = 4096
TB = 128
TSPLIT = 4
CAP = 4
HID = 384
OWNERS = 16
SLOTS = 288
META = 16
EPSILON = 1e-06
BF = jnp.bfloat16
F32 = jnp.float32
EP = ("z", "y")


HALF = CAP // 2
NAMES = ("x", "c")


def pack_kernel(owner, slot, scale, tiles, first, second, counts, meta, sems):
    held = tiles.shape[0]

    def clear(o, carry):
        counts[o] = 0
        return carry

    lax.fori_loop(0, OWNERS, clear, 0)
    meta[...] = jnp.zeros_like(meta)

    def copy(i, send, o, r):
        return pltpu.make_async_copy(tiles.at[i], send.at[o, pl.ds(r * TB, TB), :], sems.at[i])

    def place(i, carry):
        o = owner[i]
        r = counts[o]
        counts[o] = r + 1

        @pl.when(r < HALF)
        def _():
            copy(i, first, o, r).start()

        @pl.when(r >= HALF)
        def _():
            copy(i, second, o, r - HALF).start()

        code = slot[i] + 1
        value = jnp.full((1, TB), scale[i], F32)
        high = value.astype(BF).astype(F32)
        meta[o, pl.ds(r * 4, 1), :] = jnp.full((1, TB), (code // 16).astype(F32), F32)
        meta[o, pl.ds(r * 4 + 1, 1), :] = jnp.full((1, TB), (code % 16).astype(F32), F32)
        meta[o, pl.ds(r * 4 + 2, 1), :] = high
        meta[o, pl.ds(r * 4 + 3, 1), :] = value - high
        return carry

    lax.fori_loop(0, held, place, 0)
    first[:, HALF * TB :, :] = meta[...].astype(BF)

    def finish(i, carry):
        copy(i, first, 0, 0).wait()
        return carry

    lax.fori_loop(0, held, finish, 0)


def pack(owner, slot, scale, tiles):
    smem = pl.BlockSpec(memory_space=pltpu.SMEM)
    vmem = pl.BlockSpec(memory_space=pltpu.VMEM)
    held = tiles.shape[0]
    return pl.pallas_call(
        pack_kernel,
        out_shape=[
            jax.ShapeDtypeStruct((OWNERS, HALF * TB + META, TB), BF),
            jax.ShapeDtypeStruct((OWNERS, HALF * TB, TB), BF),
        ],
        in_specs=[smem, smem, smem, vmem],
        out_specs=[vmem, vmem],
        scratch_shapes=[
            pltpu.SMEM((OWNERS,), jnp.int32),
            pltpu.VMEM((OWNERS, META, TB), F32),
            pltpu.SemaphoreType.DMA((held,)),
        ],
        name="pack",
    )(owner, slot, scale, tiles)


def base_of(where, hop, other, start):
    x, c = where[0], where[1]
    return ((((x + hop) % 4) * 2 + (c + other) % 2) * OWNERS + start) * CAP


def refresh_kernel(kinds, slots, scales, where, *refs):
    blocks, (gate, up, down, both_out, down_out, delta) = refs[: len(kinds)], refs[len(kinds) :]

    def clear(s, carry):
        delta[s] = jnp.zeros((TB, TB), F32)
        return carry

    lax.fori_loop(0, SLOTS + 1, clear, 0, unroll=4)
    for (hop, other, start, half), got in zip(kinds, blocks):
        base = base_of(where, hop, other, start) + half * HALF

        def add(g, carry, got=got, base=base):
            for r in range(HALF):
                place = base + g * CAP + r
                s = slots[place]
                delta[s] += got[g, pl.ds(r * TB, TB), :].astype(F32) * scales[place]
            return carry

        lax.fori_loop(0, got.shape[0], add, 0, unroll=2)
    cols = HID // TB

    def wide(b, carry):
        for c in range(cols):
            rows, at = pl.ds(b * TB, TB), pl.ds(c * TB, TB)
            both_out[rows, at] = (gate[rows, at].astype(F32) + delta[b * cols + c]).astype(BF)
            there = pl.ds(HID + c * TB, TB)
            both_out[rows, there] = (up[rows, at].astype(F32) + delta[SLOTS // 3 + b * cols + c]).astype(BF)
            down_out[at, rows] = (
                down[at, rows].astype(F32) + delta[2 * (SLOTS // 3) + c * (D // TB) + b]
            ).astype(BF)
        return carry

    lax.fori_loop(0, D // TB, wide, 0)


def refresh(kinds, slots, scales, where, blocks, gate, up, down):
    smem = pl.BlockSpec(memory_space=pltpu.SMEM)
    vmem = pl.BlockSpec(memory_space=pltpu.VMEM)
    return pl.pallas_call(
        lambda *refs: refresh_kernel(kinds, *refs),
        out_shape=[jax.ShapeDtypeStruct((D, 2 * HID), BF), jax.ShapeDtypeStruct((HID, D), BF)],
        in_specs=[smem] * 3 + [vmem] * (len(blocks) + 3),
        out_specs=[vmem, vmem],
        scratch_shapes=[pltpu.VMEM((SLOTS + 1, TB, TB), F32)],
        compiler_params=pltpu.CompilerParams(vmem_limit_bytes=58 << 20),
        name="refresh",
    )(slots, scales, where, *blocks, gate, up, down)


def patch(kinds, slots, scales, where, blocks, both, down):
    third = SLOTS // 3
    cols = HID // TB
    for (hop, other, start, half), got in zip(kinds, blocks):
        base = base_of(where, hop, other, start) + half * HALF

        def add(g, carry, got=got, base=base):
            for r in range(HALF):
                place = base + g * CAP + r
                s = slots[place]
                tile = got.at[g, pl.ds(r * TB, TB), :]
                scale = scales[place]

                @pl.when(s < 2 * third)
                def _():
                    side = s // third
                    k = s - side * third
                    b = k // cols
                    rows = pl.ds(pl.multiple_of(b * TB, TB), TB)
                    at = pl.ds(pl.multiple_of(side * HID + (k - b * cols) * TB, TB), TB)
                    both[rows, at] = (both[rows, at].astype(F32) + tile[...].astype(F32) * scale).astype(BF)

                @pl.when((s >= 2 * third) & (s < SLOTS))
                def _():
                    k = s - 2 * third
                    b = k // (D // TB)
                    rows = pl.ds(pl.multiple_of(b * TB, TB), TB)
                    at = pl.ds(pl.multiple_of((k - b * (D // TB)) * TB, TB), TB)
                    down[rows, at] = (down[rows, at].astype(F32) + tile[...].astype(F32) * scale).astype(BF)

            return carry

        lax.fori_loop(0, got.shape[0], add, 0)


PIECE = 16
CHUNK = 1024


def gather(starts, normed, combine, block, weight, sems):
    def rows(i):
        return pl.ds(pl.multiple_of(starts[i], PIECE), PIECE), pl.ds(i * PIECE, PIECE)

    def copy(i):
        there, here = rows(i)
        return pltpu.make_async_copy(normed.at[there, :], block.at[here, :], sems.at[i])

    pieces = block.shape[0] // PIECE
    for i in range(pieces):
        copy(i).start()
    for i in range(pieces):
        there, here = rows(i)
        weight[here, :] = combine[there, :]

    def finish():
        for i in range(pieces):
            copy(i).wait()

    return finish


def multiply(block, weight, both, down, outs):
    both_part = jnp.dot(block[...], both[...], preferred_element_type=F32)
    hidden = (jax.nn.silu(both_part[:, :HID]) * both_part[:, HID:] * weight[:, :1]).astype(BF)
    for n in range(0, D, CHUNK):
        part = jnp.dot(hidden, down[:, n : n + CHUNK], preferred_element_type=F32).astype(BF)
        first = 0
        for out in outs:
            out[:, n : n + CHUNK] = part[first : first + out.shape[0]]
            first += out.shape[0]


def first_kernel(kinds, slots, scales, where, starts, normed, combine, both, down, *refs):
    blocks, refs = refs[: len(kinds)], refs[len(kinds) :]
    both_out, down_out = refs[:2]
    outs, (block, weight, sems) = refs[2:-3], refs[-3:]
    finish = gather(starts, normed, combine, block, weight, sems)

    def keep(b, carry):
        rows = pl.ds(b * TB, TB)
        both_out[rows, :] = both[rows, :]
        return carry

    lax.fori_loop(0, D // TB, keep, 0)
    down_out[...] = down[...]
    patch(kinds, slots, scales, where, blocks, both_out, down_out)
    finish()
    multiply(block, weight, both_out, down_out, outs)


def second_kernel(starts, normed, combine, both, down, *refs):
    outs, (block, weight, sems) = refs[:-3], refs[-3:]
    gather(starts, normed, combine, block, weight, sems)()
    multiply(block, weight, both, down, outs)


def scratch(rows):
    return [
        pltpu.VMEM((rows, D), BF),
        pltpu.VMEM((rows, TB), F32),
        pltpu.SemaphoreType.DMA((rows // PIECE,)),
    ]


def expert_first(kinds, slots, scales, where, starts, normed, combine, weights, blocks, parts):
    hbm = pl.BlockSpec(memory_space=pl.ANY)
    smem = pl.BlockSpec(memory_space=pltpu.SMEM)
    vmem = pl.BlockSpec(memory_space=pltpu.VMEM)
    return pl.pallas_call(
        lambda *refs: first_kernel(kinds, *refs),
        out_shape=[jax.ShapeDtypeStruct(w.shape, BF) for w in weights]
        + [jax.ShapeDtypeStruct((n, D), BF) for n in parts],
        in_specs=[smem] * 4 + [hbm, vmem, vmem, vmem] + [vmem] * len(blocks),
        out_specs=[vmem] * (2 + len(parts)),
        scratch_shapes=scratch(sum(parts)),
        compiler_params=pltpu.CompilerParams(vmem_limit_bytes=58 << 20),
        name="expert_first",
    )(slots, scales, where, starts, normed, combine, *weights, *blocks)


def expert_second(starts, normed, combine, weights, parts):
    hbm = pl.BlockSpec(memory_space=pl.ANY)
    smem = pl.BlockSpec(memory_space=pltpu.SMEM)
    vmem = pl.BlockSpec(memory_space=pltpu.VMEM)
    return pl.pallas_call(
        second_kernel,
        out_shape=[jax.ShapeDtypeStruct((n, D), BF) for n in parts],
        in_specs=[smem, hbm, vmem, vmem, vmem],
        out_specs=[vmem] * len(parts),
        scratch_shapes=scratch(sum(parts)),
        compiler_params=pltpu.CompilerParams(vmem_limit_bytes=48 << 20),
        name="expert_second",
    )(starts, normed, combine, *weights)


def shift(value, axis, by):
    n = lax.axis_size(axis)
    return lax.ppermute(value, axis, [(i, (i + by) % n) for i in range(n)])


def total(*terms):
    out = terms[0].astype(F32)
    for term in terms[1:]:
        out = out + term.astype(F32)
    return out.astype(BF)


def rows_of(half, first, second, blocks):
    first_at, second_at = lax.axis_index(first), lax.axis_index(second)
    starts = []
    for offset, quarter in blocks:
        a, b = (first_at + offset) % 4, (second_at + jnp.arange(4)) % 4
        z, y = (b, a) if first == "y" else (a, b)
        starts.append(half * (ROWS // 2) + (z * 4 + y) * 32 + quarter * PIECE)
    return jnp.concatenate(starts).astype(jnp.int32)


SENT = ((2, 0), (1, 1), (2, 1), (3, 0))
KEPT = ((1, 0), (3, 1), (0, 0), (0, 1))


def ring_sum(first, second, got_plus, got_minus, keep_plus, keep_minus, own):
    last_plus = shift(total(got_plus[:64], keep_plus), first, 1)
    last_minus = shift(total(got_minus[:64], keep_minus), first, -1)
    sums = []
    for k in range(4):
        at_k = slice(k * PIECE, (k + 1) * PIECE)
        upper = total(own[:64][at_k], got_minus[64:][at_k], last_plus[at_k])
        lower = total(own[64:][at_k], got_plus[64:][at_k], last_minus[at_k])
        sums.append(jnp.concatenate([upper, lower], axis=0))
    return total(sums[0], *(shift(sums[k], second, (1, 2, -1)[k - 1]) for k in (1, 2, 3)))


ROWS = 1024


def normalize_kernel(rows, gain, out):
    for t in range(rows.shape[1]):
        values = rows[:, t, :].astype(F32)
        scaled = values * lax.rsqrt(jnp.mean(values * values, axis=-1, keepdims=True) + EPSILON)
        out[t] = (scaled * gain[...]).astype(BF)


def normalize(hidden_rows, norm_gain):
    rows, steps, width = hidden_rows.shape
    step = 64
    return pl.pallas_call(
        normalize_kernel,
        out_shape=jax.ShapeDtypeStruct((steps, rows, width), BF),
        grid=(rows // step,),
        in_specs=[
            pl.BlockSpec((step, steps, width), lambda i: (i, 0, 0)),
            pl.BlockSpec((1, width), lambda i: (0, 0)),
        ],
        out_specs=pl.BlockSpec((steps, step, width), lambda i: (0, i, 0)),
        name="normalize",
    )(hidden_rows, norm_gain.reshape(1, width))


def tables(meta):
    fields = meta.astype(F32).reshape(OWNERS, CAP, 4)
    code = (fields[..., 0] * 16.0 + fields[..., 1]).reshape(1, -1)
    scale = (fields[..., 2] + fields[..., 3]).reshape(1, -1)
    both = lax.all_gather(jnp.concatenate([code, scale], axis=1), NAMES, axis=0, tiled=True)
    code = both[:, : OWNERS * CAP].reshape(-1).astype(jnp.int32)
    return jnp.where(code > 0, code - 1, SLOTS), both[:, OWNERS * CAP :].reshape(-1)


def other_core(value):
    return lax.ppermute(value, "c", [(0, 1), (1, 0)])


def spread(own):
    plus, minus = shift(own, "x", 1), shift(own, "x", -1)
    half = OWNERS // 2
    far_plus, far_minus = shift(plus[:half], "x", 1), shift(minus[half:], "x", -1)
    near = [(0, 0, own)]
    side = [(-1, 0, plus), (1, 0, minus)]
    far = [(2, 0, far_plus), (2, half, far_minus)]
    return [
        [(hop, core, start, v if core == 0 else other_core(v)) for hop, start, v in part for core in (0, 1)]
        for part in (near, side, far)
    ]


def body(
    hidden_rows,
    norm_gain,
    route_expert,
    route_weight,
    gate_base,
    up_base,
    down_base,
    tile_values,
    tile_scale,
    tile_owner,
    tile_slot,
):
    exchange = lambda v: lax.all_to_all(v, EP, split_axis=0, concat_axis=0, tiled=True)
    first, second = pack(tile_owner[:, 0], tile_slot, tile_scale, tile_values)
    first = exchange(first)
    slots, scales = tables(first[:, HALF * TB :, 0])
    near0, side0, far0 = spread(first)
    second = exchange(second)
    near1, side1, far1 = spread(second)
    where = jnp.stack([lax.axis_index("x"), lax.axis_index("c")]).astype(jnp.int32)
    early = [(h, c, s, 0, v) for h, c, s, v in near0 + side0 + far0] + [(h, c, s, 1, v) for h, c, s, v in near1]
    late = [(h, c, s, 1, v) for h, c, s, v in side1 + far1]
    kinds = lambda part: tuple(p[:4] for p in part)
    blocks = lambda part: [p[4] for p in part]
    weights = refresh(
        kinds(early), slots, scales, where, blocks(early), gate_base[0], up_base[0], down_base[0]
    )
    normed = normalize(hidden_rows, norm_gain).reshape(ROWS, D)
    own = lax.axis_index("z")
    combine = jnp.sum(jnp.where(route_expert == own, route_weight, 0.0), axis=-1)
    combine = jnp.broadcast_to(combine.T.reshape(ROWS, 1), (ROWS, TB))
    sent = jnp.concatenate([rows_of(0, "y", "z", SENT), rows_of(1, "z", "y", SENT)])
    kept = jnp.concatenate([rows_of(0, "y", "z", KEPT), rows_of(1, "z", "y", KEPT)])
    *weights, plus_a, minus_a, plus_b, minus_b = expert_first(
        kinds(late), slots, scales, where, sent, normed, combine, weights, blocks(late), (128,) * 4
    )
    got_a = shift(plus_a, "y", 1), shift(minus_a, "y", -1)
    got_b = shift(plus_b, "z", 1), shift(minus_b, "z", -1)
    rest = expert_second(kept, normed, combine, weights, (64, 64, 128) * 2)
    out_a = ring_sum("y", "z", *got_a, *rest[:3])
    out_b = ring_sum("z", "y", *got_b, *rest[3:])
    return jnp.stack([out_a, out_b], axis=1)


def solution(mesh):
    fine = Mesh(mesh.devices.reshape(4, 2, 4, 4), ("x", "c", "z", "y"))
    rows = ("x", "c")
    every = ("x", "c", "z", "y")
    return jax.shard_map(
        body,
        mesh=fine,
        in_specs=(
            P(rows, None, None),
            P(),
            P(rows, None, None),
            P(rows, None, None),
            P(EP, None, None),
            P(EP, None, None),
            P(EP, None, None),
            P(every, None, None),
            P(every),
            P(every, None),
            P(every),
        ),
        out_specs=P(every, None, None),
        check_vma=False,
    )
```

```python
import jax
import jax.numpy as jnp
from jax import lax
from jax.experimental import pallas as pl
from jax.experimental.pallas import tpu as pltpu
from jax.sharding import Mesh, PartitionSpec as P

D = 4096
TB = 128
TSPLIT = 4
CAP = 4
HID = 384
OWNERS = 16
SLOTS = 288
META = 16
EPSILON = 1e-06
BF = jnp.bfloat16
F32 = jnp.float32
EP = ("z", "y")


HALF = CAP // 2
NAMES = ("x", "c")


def cost(us, moved=0):
    return pl.CostEstimate(flops=int(us * 1e9), transcendentals=0, bytes_accessed=moved)


def pack_kernel(owner, slot, scale, tiles, first, second, counts, meta, sems):
    held = tiles.shape[0]

    def clear(o, carry):
        counts[o] = 0
        return carry

    lax.fori_loop(0, OWNERS, clear, 0)
    meta[...] = jnp.zeros_like(meta)

    def copy(i, send, o, r):
        return pltpu.make_async_copy(tiles.at[i], send.at[o, pl.ds(r * TB, TB), :], sems.at[i])

    def place(i, carry):
        o = owner[i]
        r = counts[o]
        counts[o] = r + 1

        @pl.when(r < HALF)
        def _():
            copy(i, first, o, r).start()

        @pl.when(r >= HALF)
        def _():
            copy(i, second, o, r - HALF).start()

        code = slot[i] + 1
        value = jnp.full((1, TB), scale[i], F32)
        high = value.astype(BF).astype(F32)
        meta[o, pl.ds(r * 4, 1), :] = jnp.full((1, TB), (code // 16).astype(F32), F32)
        meta[o, pl.ds(r * 4 + 1, 1), :] = jnp.full((1, TB), (code % 16).astype(F32), F32)
        meta[o, pl.ds(r * 4 + 2, 1), :] = high
        meta[o, pl.ds(r * 4 + 3, 1), :] = value - high
        return carry

    lax.fori_loop(0, held, place, 0)
    first[:, HALF * TB :, :] = meta[...].astype(BF)

    def finish(i, carry):
        copy(i, first, 0, 0).wait()
        return carry

    lax.fori_loop(0, held, finish, 0)


def pack(owner, slot, scale, tiles):
    smem = pl.BlockSpec(memory_space=pltpu.SMEM)
    vmem = pl.BlockSpec(memory_space=pltpu.VMEM)
    held = tiles.shape[0]
    return pl.pallas_call(
        pack_kernel,
        out_shape=[
            jax.ShapeDtypeStruct((OWNERS, HALF * TB + META, TB), BF),
            jax.ShapeDtypeStruct((OWNERS, HALF * TB, TB), BF),
        ],
        in_specs=[smem, smem, smem, vmem],
        out_specs=[vmem, vmem],
        scratch_shapes=[
            pltpu.SMEM((OWNERS,), jnp.int32),
            pltpu.VMEM((OWNERS, META, TB), F32),
            pltpu.SemaphoreType.DMA((held,)),
        ],
        cost_estimate=cost(5),
        name="pack",
    )(owner, slot, scale, tiles)


def base_of(where, hop, other, start):
    x, c = where[0], where[1]
    return ((((x + hop) % 4) * 2 + (c + other) % 2) * OWNERS + start) * CAP


def refresh_kernel(kinds, slots, scales, where, *refs):
    blocks, (gate, up, down, both_out, down_out, delta) = refs[: len(kinds)], refs[len(kinds) :]

    def clear(s, carry):
        delta[s] = jnp.zeros((TB, TB), F32)
        return carry

    lax.fori_loop(0, SLOTS + 1, clear, 0, unroll=4)
    for (hop, other, start, half), got in zip(kinds, blocks):
        base = base_of(where, hop, other, start) + half * HALF

        def add(g, carry, got=got, base=base):
            for r in range(HALF):
                place = base + g * CAP + r
                s = slots[place]
                delta[s] += got[g, pl.ds(r * TB, TB), :].astype(F32) * scales[place]
            return carry

        lax.fori_loop(0, got.shape[0], add, 0, unroll=2)
    cols = HID // TB

    def wide(b, carry):
        for c in range(cols):
            rows, at = pl.ds(b * TB, TB), pl.ds(c * TB, TB)
            both_out[rows, at] = (gate[rows, at].astype(F32) + delta[b * cols + c]).astype(BF)
            there = pl.ds(HID + c * TB, TB)
            both_out[rows, there] = (up[rows, at].astype(F32) + delta[SLOTS // 3 + b * cols + c]).astype(BF)
            down_out[at, rows] = (
                down[at, rows].astype(F32) + delta[2 * (SLOTS // 3) + c * (D // TB) + b]
            ).astype(BF)
        return carry

    lax.fori_loop(0, D // TB, wide, 0)


def refresh(kinds, slots, scales, where, blocks, gate, up, down):
    smem = pl.BlockSpec(memory_space=pltpu.SMEM)
    vmem = pl.BlockSpec(memory_space=pltpu.VMEM)
    return pl.pallas_call(
        lambda *refs: refresh_kernel(kinds, *refs),
        out_shape=[jax.ShapeDtypeStruct((D, 2 * HID), BF), jax.ShapeDtypeStruct((HID, D), BF)],
        in_specs=[smem] * 3 + [vmem] * (len(blocks) + 3),
        out_specs=[vmem, vmem],
        scratch_shapes=[pltpu.VMEM((SLOTS + 1, TB, TB), F32)],
        compiler_params=pltpu.CompilerParams(vmem_limit_bytes=58 << 20),
        cost_estimate=cost(17),
        name="refresh",
    )(slots, scales, where, *blocks, gate, up, down)


def patch(kinds, slots, scales, where, blocks, both, down):
    third = SLOTS // 3
    cols = HID // TB
    for (hop, other, start, half), got in zip(kinds, blocks):
        base = base_of(where, hop, other, start) + half * HALF

        def add(g, carry, got=got, base=base):
            for r in range(HALF):
                place = base + g * CAP + r
                s = slots[place]
                tile = got.at[g, pl.ds(r * TB, TB), :]
                scale = scales[place]

                @pl.when(s < 2 * third)
                def _():
                    side = s // third
                    k = s - side * third
                    b = k // cols
                    rows = pl.ds(pl.multiple_of(b * TB, TB), TB)
                    at = pl.ds(pl.multiple_of(side * HID + (k - b * cols) * TB, TB), TB)
                    both[rows, at] = (both[rows, at].astype(F32) + tile[...].astype(F32) * scale).astype(BF)

                @pl.when((s >= 2 * third) & (s < SLOTS))
                def _():
                    k = s - 2 * third
                    b = k // (D // TB)
                    rows = pl.ds(pl.multiple_of(b * TB, TB), TB)
                    at = pl.ds(pl.multiple_of((k - b * (D // TB)) * TB, TB), TB)
                    down[rows, at] = (down[rows, at].astype(F32) + tile[...].astype(F32) * scale).astype(BF)

            return carry

        lax.fori_loop(0, got.shape[0], add, 0)


PIECE = 16
CHUNK = 1024


def gather(starts, normed, combine, block, weight, sems):
    def rows(i):
        return pl.ds(pl.multiple_of(starts[i], PIECE), PIECE), pl.ds(i * PIECE, PIECE)

    def copy(i):
        there, here = rows(i)
        return pltpu.make_async_copy(normed.at[there, :], block.at[here, :], sems.at[i])

    pieces = block.shape[0] // PIECE
    for i in range(pieces):
        copy(i).start()
    for i in range(pieces):
        there, here = rows(i)
        weight[here, :] = combine[there, :]

    def finish():
        for i in range(pieces):
            copy(i).wait()

    return finish


def multiply(block, weight, both, down, outs):
    both_part = jnp.dot(block[...], both[...], preferred_element_type=F32)
    hidden = (jax.nn.silu(both_part[:, :HID]) * both_part[:, HID:] * weight[:, :1]).astype(BF)
    for n in range(0, D, CHUNK):
        part = jnp.dot(hidden, down[:, n : n + CHUNK], preferred_element_type=F32).astype(BF)
        first = 0
        for out in outs:
            out[:, n : n + CHUNK] = part[first : first + out.shape[0]]
            first += out.shape[0]


def keep(both, down, both_out, down_out):
    def copy(b, carry):
        rows = pl.ds(b * TB, TB)
        both_out[rows, :] = both[rows, :]
        return carry

    lax.fori_loop(0, D // TB, copy, 0)
    down_out[...] = down[...]


def first_kernel(kinds, slots, scales, where, starts, normed, combine, both, down, *refs):
    blocks, refs = refs[: len(kinds)], refs[len(kinds) :]
    both_out, down_out = refs[:2]
    outs, (block, weight, sems) = refs[2:-3], refs[-3:]
    finish = gather(starts, normed, combine, block, weight, sems)

    keep(both, down, both_out, down_out)
    patch(kinds, slots, scales, where, blocks, both_out, down_out)
    finish()
    multiply(block, weight, both_out, down_out, outs)


def add_kernel(kinds, slots, scales, where, both, down, *refs):
    blocks, (both_out, down_out) = refs[: len(kinds)], refs[len(kinds) :]
    keep(both, down, both_out, down_out)
    patch(kinds, slots, scales, where, blocks, both_out, down_out)


def add_tiles(kinds, slots, scales, where, weights, blocks):
    smem = pl.BlockSpec(memory_space=pltpu.SMEM)
    vmem = pl.BlockSpec(memory_space=pltpu.VMEM)
    return pl.pallas_call(
        lambda *refs: add_kernel(kinds, *refs),
        out_shape=[jax.ShapeDtypeStruct(w.shape, BF) for w in weights],
        in_specs=[smem] * 3 + [vmem] * (2 + len(blocks)),
        out_specs=[vmem] * 2,
        compiler_params=pltpu.CompilerParams(vmem_limit_bytes=40 << 20),
        cost_estimate=cost(7),
        name="add_tiles",
    )(slots, scales, where, *weights, *blocks)


def second_kernel(starts, normed, combine, both, down, *refs):
    outs, (block, weight, sems) = refs[:-3], refs[-3:]
    gather(starts, normed, combine, block, weight, sems)()
    multiply(block, weight, both, down, outs)


def scratch(rows):
    return [
        pltpu.VMEM((rows, D), BF),
        pltpu.VMEM((rows, TB), F32),
        pltpu.SemaphoreType.DMA((rows // PIECE,)),
    ]


def expert_first(kinds, slots, scales, where, starts, normed, combine, weights, blocks, parts):
    hbm = pl.BlockSpec(memory_space=pl.ANY)
    smem = pl.BlockSpec(memory_space=pltpu.SMEM)
    vmem = pl.BlockSpec(memory_space=pltpu.VMEM)
    return pl.pallas_call(
        lambda *refs: first_kernel(kinds, *refs),
        out_shape=[jax.ShapeDtypeStruct(w.shape, BF) for w in weights]
        + [jax.ShapeDtypeStruct((n, D), BF) for n in parts],
        in_specs=[smem] * 4 + [hbm, vmem, vmem, vmem] + [vmem] * len(blocks),
        out_specs=[vmem] * (2 + len(parts)),
        scratch_shapes=scratch(sum(parts)),
        compiler_params=pltpu.CompilerParams(vmem_limit_bytes=58 << 20),
        cost_estimate=cost(18),
        name="expert_first",
    )(slots, scales, where, starts, normed, combine, *weights, *blocks)


def expert_second(starts, normed, combine, weights, parts):
    hbm = pl.BlockSpec(memory_space=pl.ANY)
    smem = pl.BlockSpec(memory_space=pltpu.SMEM)
    vmem = pl.BlockSpec(memory_space=pltpu.VMEM)
    return pl.pallas_call(
        second_kernel,
        out_shape=[jax.ShapeDtypeStruct((n, D), BF) for n in parts],
        in_specs=[smem, hbm, vmem, vmem, vmem],
        out_specs=[vmem] * len(parts),
        scratch_shapes=scratch(sum(parts)),
        compiler_params=pltpu.CompilerParams(vmem_limit_bytes=48 << 20),
        cost_estimate=cost(14),
        name="expert_second",
    )(starts, normed, combine, *weights)


def shift(value, axis, by):
    n = lax.axis_size(axis)
    return lax.ppermute(value, axis, [(i, (i + by) % n) for i in range(n)])


def total(*terms):
    out = terms[0].astype(F32)
    for term in terms[1:]:
        out = out + term.astype(F32)
    return out.astype(BF)


def rows_of(half, first, second, blocks):
    first_at, second_at = lax.axis_index(first), lax.axis_index(second)
    starts = []
    for offset, quarter in blocks:
        a, b = (first_at + offset) % 4, (second_at + jnp.arange(4)) % 4
        z, y = (b, a) if first == "y" else (a, b)
        starts.append(half * (ROWS // 2) + (z * 4 + y) * 32 + quarter * PIECE)
    return jnp.concatenate(starts).astype(jnp.int32)


SENT = ((2, 0), (1, 1), (2, 1), (3, 0))
KEPT = ((1, 0), (3, 1), (0, 0), (0, 1))


def ring_sum(first, second, got_plus, got_minus, keep_plus, keep_minus, own):
    last_plus = shift(total(got_plus[:64], keep_plus), first, 1)
    last_minus = shift(total(got_minus[:64], keep_minus), first, -1)
    sums = []
    for k in range(4):
        at_k = slice(k * PIECE, (k + 1) * PIECE)
        upper = total(own[:64][at_k], got_minus[64:][at_k], last_plus[at_k])
        lower = total(own[64:][at_k], got_plus[64:][at_k], last_minus[at_k])
        sums.append(jnp.concatenate([upper, lower], axis=0))
    return total(sums[0], *(shift(sums[k], second, (1, 2, -1)[k - 1]) for k in (1, 2, 3)))


ROWS = 1024


def normalize_kernel(rows, gain, out):
    for t in range(rows.shape[1]):
        values = rows[:, t, :].astype(F32)
        scaled = values * lax.rsqrt(jnp.mean(values * values, axis=-1, keepdims=True) + EPSILON)
        out[t] = (scaled * gain[...]).astype(BF)


def normalize(hidden_rows, norm_gain):
    rows, steps, width = hidden_rows.shape
    step = 64
    return pl.pallas_call(
        normalize_kernel,
        out_shape=jax.ShapeDtypeStruct((steps, rows, width), BF),
        grid=(rows // step,),
        in_specs=[
            pl.BlockSpec((step, steps, width), lambda i: (i, 0, 0)),
            pl.BlockSpec((1, width), lambda i: (0, 0)),
        ],
        out_specs=pl.BlockSpec((steps, step, width), lambda i: (0, i, 0)),
        cost_estimate=cost(18),
        name="normalize",
    )(hidden_rows, norm_gain.reshape(1, width))


def tables(meta):
    fields = meta.astype(F32).reshape(OWNERS, CAP, 4)
    code = (fields[..., 0] * 16.0 + fields[..., 1]).reshape(1, -1)
    scale = (fields[..., 2] + fields[..., 3]).reshape(1, -1)
    both = lax.all_gather(jnp.concatenate([code, scale], axis=1), NAMES, axis=0, tiled=True)
    code = both[:, : OWNERS * CAP].reshape(-1).astype(jnp.int32)
    return jnp.where(code > 0, code - 1, SLOTS), both[:, OWNERS * CAP :].reshape(-1)


def other_core(value):
    return lax.ppermute(value, "c", [(0, 1), (1, 0)])


def pinned(value, *others):
    return lax.optimization_barrier((value, *others))[0]


def both_cores(hop, start, value):
    return [(hop, 0, start, value), (hop, 1, start, other_core(value))]


def from_neighbours(own):
    return shift(own, "x", 1), shift(own, "x", -1)


def from_far(plus, minus):
    half = OWNERS // 2
    return shift(plus[:half], "x", 1), shift(minus[half:], "x", -1)


def near_blocks(own):
    return both_cores(0, 0, own)


def side_blocks(plus, minus):
    return both_cores(-1, 0, plus) + both_cores(1, 0, minus)


def far_blocks(plus, minus):
    return both_cores(2, 0, plus) + both_cores(2, OWNERS // 2, minus)


def body(
    hidden_rows,
    norm_gain,
    route_expert,
    route_weight,
    gate_base,
    up_base,
    down_base,
    tile_values,
    tile_scale,
    tile_owner,
    tile_slot,
):
    exchange = lambda v: lax.all_to_all(v, EP, split_axis=0, concat_axis=0, tiled=True)
    first, second = pack(tile_owner[:, 0], tile_slot, tile_scale, tile_values)
    first = exchange(first)
    slots, scales = tables(first[:, HALF * TB :, 0])
    side0 = from_neighbours(first)
    near0 = near_blocks(first)
    second = exchange(second)
    normed = normalize(hidden_rows, norm_gain).reshape(ROWS, D)
    side0 = [pinned(v, normed, slots, scales) for v in side0]
    far0 = from_far(*side0)
    side1 = from_neighbours(pinned(second, *side0))
    early = near0 + side_blocks(*side0) + far_blocks(*far0)
    early = [(h, c, s, 0, v) for h, c, s, v in early] + [(h, c, s, 1, v) for h, c, s, v in near_blocks(second)]
    middle = [(h, c, s, 1, v) for h, c, s, v in side_blocks(*side1)]
    late = [(h, c, s, 1, v) for h, c, s, v in far_blocks(*from_far(*side1))]
    where = jnp.stack([lax.axis_index("x"), lax.axis_index("c")]).astype(jnp.int32)
    kinds = lambda part: tuple(p[:4] for p in part)
    blocks = lambda part: [p[4] for p in part]
    weights = refresh(
        kinds(early), slots, scales, where, blocks(early), gate_base[0], up_base[0], down_base[0]
    )
    weights = add_tiles(kinds(middle), slots, scales, where, weights, blocks(middle))
    own = lax.axis_index("z")
    combine = jnp.sum(jnp.where(route_expert == own, route_weight, 0.0), axis=-1)
    combine = jnp.broadcast_to(combine.T.reshape(ROWS, 1), (ROWS, TB))
    sent = jnp.concatenate([rows_of(0, "y", "z", SENT), rows_of(1, "z", "y", SENT)])
    kept = jnp.concatenate([rows_of(0, "y", "z", KEPT), rows_of(1, "z", "y", KEPT)])
    *weights, plus_a, minus_a, plus_b, minus_b = expert_first(
        kinds(late), slots, scales, where, sent, normed, combine, weights, blocks(late), (128,) * 4
    )
    got_a = shift(plus_a, "y", 1), shift(minus_a, "y", -1)
    got_b = shift(plus_b, "z", 1), shift(minus_b, "z", -1)
    rest = expert_second(kept, normed, combine, weights, (64, 64, 128) * 2)
    out_a = ring_sum("y", "z", *got_a, *rest[:3])
    out_b = ring_sum("z", "y", *got_b, *rest[3:])
    return jnp.stack([out_a, out_b], axis=1)


def solution(mesh):
    fine = Mesh(mesh.devices.reshape(4, 2, 4, 4), ("x", "c", "z", "y"))
    rows = ("x", "c")
    every = ("x", "c", "z", "y")
    return jax.shard_map(
        body,
        mesh=fine,
        in_specs=(
            P(rows, None, None),
            P(),
            P(rows, None, None),
            P(rows, None, None),
            P(EP, None, None),
            P(EP, None, None),
            P(EP, None, None),
            P(every, None, None),
            P(every),
            P(every, None),
            P(every),
        ),
        out_specs=P(every, None, None),
        check_vma=False,
    )
```

```python
import jax
import jax.numpy as jnp
from jax import lax
from jax.experimental import pallas as pl
from jax.experimental.pallas import tpu as pltpu
from jax.sharding import Mesh, PartitionSpec as P

D = 4096
TB = 128
TSPLIT = 4
CAP = 4
HID = 384
OWNERS = 16
SLOTS = 288
META = 16
EPSILON = 1e-06
BF = jnp.bfloat16
F32 = jnp.float32
EP = ("z", "y")


HALF = CAP // 2
NAMES = ("x", "c")


def cost(us, moved=0):
    return pl.CostEstimate(flops=int(us * 1e9), transcendentals=0, bytes_accessed=moved)


def pack_kernel(owner, slot, scale, tiles, first, second, counts, meta, sems):
    held = tiles.shape[0]

    def clear(o, carry):
        counts[o] = 0
        return carry

    lax.fori_loop(0, OWNERS, clear, 0)
    meta[...] = jnp.zeros_like(meta)

    def copy(i, send, o, r):
        return pltpu.make_async_copy(tiles.at[i], send.at[o, pl.ds(r * TB, TB), :], sems.at[i])

    def place(i, carry):
        o = owner[i]
        r = counts[o]
        counts[o] = r + 1

        @pl.when(r < HALF)
        def _():
            copy(i, first, o, r).start()

        @pl.when(r >= HALF)
        def _():
            copy(i, second, o, r - HALF).start()

        code = slot[i] + 1
        value = jnp.full((1, TB), scale[i], F32)
        high = value.astype(BF).astype(F32)
        meta[o, pl.ds(r * 4, 1), :] = jnp.full((1, TB), (code // 16).astype(F32), F32)
        meta[o, pl.ds(r * 4 + 1, 1), :] = jnp.full((1, TB), (code % 16).astype(F32), F32)
        meta[o, pl.ds(r * 4 + 2, 1), :] = high
        meta[o, pl.ds(r * 4 + 3, 1), :] = value - high
        return carry

    lax.fori_loop(0, held, place, 0)
    first[:, HALF * TB :, :] = meta[...].astype(BF)

    def finish(i, carry):
        copy(i, first, 0, 0).wait()
        return carry

    lax.fori_loop(0, held, finish, 0)


def pack(owner, slot, scale, tiles):
    smem = pl.BlockSpec(memory_space=pltpu.SMEM)
    vmem = pl.BlockSpec(memory_space=pltpu.VMEM)
    held = tiles.shape[0]
    return pl.pallas_call(
        pack_kernel,
        out_shape=[
            jax.ShapeDtypeStruct((OWNERS, HALF * TB + META, TB), BF),
            jax.ShapeDtypeStruct((OWNERS, HALF * TB, TB), BF),
        ],
        in_specs=[smem, smem, smem, vmem],
        out_specs=[vmem, vmem],
        scratch_shapes=[
            pltpu.SMEM((OWNERS,), jnp.int32),
            pltpu.VMEM((OWNERS, META, TB), F32),
            pltpu.SemaphoreType.DMA((held,)),
        ],
        cost_estimate=cost(5),
        name="pack",
    )(owner, slot, scale, tiles)


def base_of(where, hop, other, start):
    x, c = where[0], where[1]
    return ((((x + hop) % 4) * 2 + (c + other) % 2) * OWNERS + start) * CAP


def refresh_kernel(kinds, slots, scales, where, *refs):
    blocks, (gate, up, down, both_out, down_out, delta) = refs[: len(kinds)], refs[len(kinds) :]

    def clear(s, carry):
        delta[s] = jnp.zeros((TB, TB), F32)
        return carry

    lax.fori_loop(0, SLOTS + 1, clear, 0, unroll=4)
    for (hop, other, start, half), got in zip(kinds, blocks):
        base = base_of(where, hop, other, start) + half * HALF

        def add(g, carry, got=got, base=base):
            for r in range(HALF):
                place = base + g * CAP + r
                s = slots[place]
                delta[s] += got[g, pl.ds(r * TB, TB), :].astype(F32) * scales[place]
            return carry

        lax.fori_loop(0, got.shape[0], add, 0, unroll=2)
    cols = HID // TB

    def wide(b, carry):
        for c in range(cols):
            rows, at = pl.ds(b * TB, TB), pl.ds(c * TB, TB)
            both_out[rows, at] = (gate[rows, at].astype(F32) + delta[b * cols + c]).astype(BF)
            there = pl.ds(HID + c * TB, TB)
            both_out[rows, there] = (up[rows, at].astype(F32) + delta[SLOTS // 3 + b * cols + c]).astype(BF)
            down_out[at, rows] = (
                down[at, rows].astype(F32) + delta[2 * (SLOTS // 3) + c * (D // TB) + b]
            ).astype(BF)
        return carry

    lax.fori_loop(0, D // TB, wide, 0)


def refresh(kinds, slots, scales, where, blocks, gate, up, down):
    smem = pl.BlockSpec(memory_space=pltpu.SMEM)
    vmem = pl.BlockSpec(memory_space=pltpu.VMEM)
    return pl.pallas_call(
        lambda *refs: refresh_kernel(kinds, *refs),
        out_shape=[pltpu.HBM((D, 2 * HID), BF), pltpu.HBM((HID, D), BF)],
        in_specs=[smem] * 3 + [vmem] * (len(blocks) + 3),
        out_specs=[vmem, vmem],
        scratch_shapes=[pltpu.VMEM((SLOTS + 1, TB, TB), F32)],
        compiler_params=pltpu.CompilerParams(vmem_limit_bytes=58 << 20),
        cost_estimate=cost(17),
        name="refresh",
    )(slots, scales, where, *blocks, gate, up, down)


def patch(kinds, slots, scales, where, blocks, both, down):
    third = SLOTS // 3
    cols = HID // TB
    for (hop, other, start, half), got in zip(kinds, blocks):
        base = base_of(where, hop, other, start) + half * HALF

        def add(g, carry, got=got, base=base):
            for r in range(HALF):
                place = base + g * CAP + r
                s = slots[place]
                tile = got.at[g, pl.ds(r * TB, TB), :]
                scale = scales[place]

                @pl.when(s < 2 * third)
                def _():
                    side = s // third
                    k = s - side * third
                    b = k // cols
                    rows = pl.ds(pl.multiple_of(b * TB, TB), TB)
                    at = pl.ds(pl.multiple_of(side * HID + (k - b * cols) * TB, TB), TB)
                    both[rows, at] = (both[rows, at].astype(F32) + tile[...].astype(F32) * scale).astype(BF)

                @pl.when((s >= 2 * third) & (s < SLOTS))
                def _():
                    k = s - 2 * third
                    b = k // (D // TB)
                    rows = pl.ds(pl.multiple_of(b * TB, TB), TB)
                    at = pl.ds(pl.multiple_of((k - b * (D // TB)) * TB, TB), TB)
                    down[rows, at] = (down[rows, at].astype(F32) + tile[...].astype(F32) * scale).astype(BF)

            return carry

        lax.fori_loop(0, got.shape[0], add, 0)


PIECE = 16
CHUNK = 512
BLOCK = 256


def in_hbm(values):
    return [pltpu.with_memory_space_constraint(v, pltpu.HBM) for v in values]


def load(pairs, sems):
    copies = [pltpu.make_async_copy(src, dst, sems.at[i]) for i, (src, dst) in enumerate(pairs)]
    for copy in copies:
        copy.start()
    return copies


def expert_kernel(kinds, parts, slots, scales, where, rows, weight, both_in, down_in, *refs):
    blocks, outs = refs[: len(kinds)], refs[len(kinds) : len(kinds) + len(parts)]
    both, down, held, sems, out_sems = refs[len(kinds) + len(parts) :]
    for copy in load(((both_in, both), (down_in, down)), sems):
        copy.wait()
    patch(kinds, slots, scales, where, blocks, both, down)
    first, copies = 0, []
    starts = [sum(parts[:i]) for i in range(len(parts))]
    while first < sum(parts):
        here = slice(first, first + BLOCK)
        part = jnp.dot(rows[here, :], both[...], preferred_element_type=F32)
        hidden = (jax.nn.silu(part[:, :HID]) * part[:, HID:] * weight[here, :1]).astype(BF)
        for n in range(0, D, CHUNK):
            at = slice(n, n + CHUNK)
            held[here, at] = jnp.dot(hidden, down[:, at], preferred_element_type=F32).astype(BF)
        for i, start in enumerate(starts):
            if first <= start < first + BLOCK:
                copy = pltpu.make_async_copy(held.at[start : start + parts[i], :], outs[i], out_sems.at[i])
                copy.start()
                copies.append(copy)
        first += BLOCK
    for copy in copies:
        copy.wait()


def expert(kinds, slots, scales, where, rows, weight, weights, blocks, parts, name):
    hbm = pl.BlockSpec(memory_space=pltpu.HBM)
    smem = pl.BlockSpec(memory_space=pltpu.SMEM)
    vmem = pl.BlockSpec(memory_space=pltpu.VMEM)
    return pl.pallas_call(
        lambda *refs: expert_kernel(kinds, parts, *refs),
        out_shape=[jax.ShapeDtypeStruct((n, D), BF) for n in parts],
        in_specs=[smem] * 3 + [vmem, vmem, hbm, hbm] + [vmem] * len(blocks),
        out_specs=[pl.BlockSpec(memory_space=pl.ANY)] * len(parts),
        scratch_shapes=[pltpu.VMEM(w.shape, BF) for w in weights]
        + [
            pltpu.VMEM((sum(parts), D), BF),
            pltpu.SemaphoreType.DMA((2,)),
            pltpu.SemaphoreType.DMA((len(parts),)),
        ],
        compiler_params=pltpu.CompilerParams(vmem_limit_bytes=36 << 20),
        cost_estimate=cost(13),
        name=name,
    )(slots, scales, where, rows, weight, *in_hbm(weights), *blocks)


def add_kernel(kinds, slots, scales, where, both_in, down_in, *refs):
    blocks, (both_out, down_out, both, down, sems) = refs[: len(kinds)], refs[len(kinds) :]
    for copy in load(((both_in, both), (down_in, down)), sems):
        copy.wait()
    patch(kinds, slots, scales, where, blocks, both, down)
    for copy in load(((both, both_out), (down, down_out)), sems):
        copy.wait()


def add_tiles(kinds, slots, scales, where, weights, blocks):
    hbm = pl.BlockSpec(memory_space=pltpu.HBM)
    smem = pl.BlockSpec(memory_space=pltpu.SMEM)
    vmem = pl.BlockSpec(memory_space=pltpu.VMEM)
    return pl.pallas_call(
        lambda *refs: add_kernel(kinds, *refs),
        out_shape=[pltpu.HBM(w.shape, BF) for w in weights],
        in_specs=[smem] * 3 + [hbm] * 2 + [vmem] * len(blocks),
        out_specs=[hbm] * 2,
        scratch_shapes=[pltpu.VMEM(w.shape, BF) for w in weights] + [pltpu.SemaphoreType.DMA((2,))],
        compiler_params=pltpu.CompilerParams(vmem_limit_bytes=24 << 20),
        cost_estimate=cost(8),
        name="add_tiles",
    )(slots, scales, where, *in_hbm(weights), *blocks)


def shift(value, axis, by):
    n = lax.axis_size(axis)
    return lax.ppermute(value, axis, [(i, (i + by) % n) for i in range(n)])


def total(*terms):
    out = terms[0].astype(F32)
    for term in terms[1:]:
        out = out + term.astype(F32)
    return out.astype(BF)


def ring_sum(first, second, got_plus, got_minus, keep_plus, keep_minus, own):
    last_plus = shift(total(got_plus[:64], keep_plus), first, 1)
    last_minus = shift(total(got_minus[:64], keep_minus), first, -1)
    sums = []
    for k in range(4):
        at_k = slice(k * PIECE, (k + 1) * PIECE)
        upper = total(own[:64][at_k], got_minus[64:][at_k], last_plus[at_k])
        lower = total(own[64:][at_k], got_plus[64:][at_k], last_minus[at_k])
        sums.append(jnp.concatenate([upper, lower], axis=0))
    return total(sums[0], *(shift(sums[k], second, (1, 2, -1)[k - 1]) for k in (1, 2, 3)))


DEST = 32
QUARTER = 8
PLACES = ((1, 2), (1, 3), (1, 0), (0, 1), (0, 0), (0, 2), (0, 3), (1, 1))


def normalize_kernel(at, rows, combine, gain, sent, kept, sent_weight, kept_weight):
    count, steps, width = rows.shape
    values = rows[...].reshape(count * steps, width).astype(F32)
    scaled = values * lax.rsqrt(jnp.mean(values * values, axis=-1, keepdims=True) + EPSILON)
    scaled = (scaled * gain[...]).astype(BF)
    weight = jnp.broadcast_to(combine[...], (count * steps, TB))
    z_at, y_at = at[0], at[1]
    for piece in range(count // QUARTER):
        owner = pl.program_id(0) * (count // DEST) + piece // (DEST // QUARTER)
        z, y = (owner // 4 + 4 - z_at) % 4, (owner % 4 + 4 - y_at) % 4
        half, quarter = piece % 4 // 2, piece % 2
        offset, k = (y, z) if half == 0 else (z, y)
        here = slice(piece * PIECE, (piece + 1) * PIECE)
        for o in range(4):
            kind, place = PLACES[o * 2 + quarter]
            there = pl.ds(pl.multiple_of(half * 256 + place * 64 + k * PIECE, PIECE), PIECE)

            @pl.when(offset == o)
            def _():
                (sent, kept)[kind][there, :] = scaled[here]
                (sent_weight, kept_weight)[kind][there, :] = weight[here]


def normalize(at, hidden_rows, combine, norm_gain):
    rows, steps, width = hidden_rows.shape
    step = 64
    half = rows * steps // 2
    whole = lambda n: pl.BlockSpec((half, n), lambda i, *_: (0, 0), pipeline_mode=pl.Buffered(1))
    return pl.pallas_call(
        normalize_kernel,
        out_shape=[pltpu.HBM((half, width), BF)] * 2 + [pltpu.HBM((half, TB), F32)] * 2,
        grid_spec=pltpu.PrefetchScalarGridSpec(
            num_scalar_prefetch=1,
            grid=(rows // step,),
            in_specs=[
                pl.BlockSpec((step, steps, width), lambda i, *_: (i, 0, 0)),
                pl.BlockSpec((step * steps, 1), lambda i, *_: (i, 0)),
                pl.BlockSpec((1, width), lambda i, *_: (0, 0)),
            ],
            out_specs=[whole(width), whole(width), whole(TB), whole(TB)],
        ),
        compiler_params=pltpu.CompilerParams(dimension_semantics=("arbitrary",), vmem_limit_bytes=32 << 20),
        cost_estimate=cost(15),
        name="normalize",
    )(at, pltpu.with_memory_space_constraint(hidden_rows, pltpu.HBM), combine, norm_gain.reshape(1, width))


def tables(meta):
    fields = meta.astype(F32).reshape(OWNERS, CAP, 4)
    code = (fields[..., 0] * 16.0 + fields[..., 1]).reshape(1, -1)
    scale = (fields[..., 2] + fields[..., 3]).reshape(1, -1)
    both = lax.all_gather(jnp.concatenate([code, scale], axis=1), NAMES, axis=0, tiled=True)
    code = both[:, : OWNERS * CAP].reshape(-1).astype(jnp.int32)
    return jnp.where(code > 0, code - 1, SLOTS), both[:, OWNERS * CAP :].reshape(-1)


def other_core(value):
    return lax.ppermute(value, "c", [(0, 1), (1, 0)])


def pinned(value, *others):
    return lax.optimization_barrier((value, *others))[0]


def both_cores(hop, start, value):
    return [(hop, 0, start, value), (hop, 1, start, other_core(value))]


def from_neighbours(own):
    return shift(own, "x", 1), shift(own, "x", -1)


def from_far(plus, minus):
    half = OWNERS // 2
    return shift(plus[:half], "x", 1), shift(minus[half:], "x", -1)


def near_blocks(own):
    return both_cores(0, 0, own)


def side_blocks(plus, minus):
    return both_cores(-1, 0, plus) + both_cores(1, 0, minus)


def far_blocks(plus, minus):
    return both_cores(2, 0, plus) + both_cores(2, OWNERS // 2, minus)


def body(
    hidden_rows,
    norm_gain,
    route_expert,
    route_weight,
    gate_base,
    up_base,
    down_base,
    tile_values,
    tile_scale,
    tile_owner,
    tile_slot,
):
    exchange = lambda v: lax.all_to_all(v, EP, split_axis=0, concat_axis=0, tiled=True)
    first, second = pack(tile_owner[:, 0], tile_slot, tile_scale, tile_values)
    first = exchange(first)
    slots, scales = tables(first[:, HALF * TB :, 0])
    side0 = from_neighbours(first)
    near0 = near_blocks(first)
    second = exchange(second)
    own = lax.axis_index("z")
    combine = jnp.sum(jnp.where(route_expert == own, route_weight, 0.0), axis=-1).reshape(-1, 1)
    at = jnp.stack([own, lax.axis_index("y")]).astype(jnp.int32)
    sent, kept, sent_weight, kept_weight = normalize(at, hidden_rows, combine, norm_gain)
    side0 = [pinned(v, sent, slots, scales) for v in side0]
    far0 = from_far(*side0)
    side1 = from_neighbours(pinned(second, *side0))
    early = near0 + side_blocks(*side0) + far_blocks(*far0)
    early = [(h, c, s, 0, v) for h, c, s, v in early] + [(h, c, s, 1, v) for h, c, s, v in near_blocks(second)]
    where = jnp.stack([lax.axis_index("x"), lax.axis_index("c")]).astype(jnp.int32)
    kinds = lambda part: tuple(p[:4] for p in part)
    blocks = lambda part: [p[4] for p in part]
    weights = refresh(
        kinds(early), slots, scales, where, blocks(early), gate_base[0], up_base[0], down_base[0]
    )
    side1 = [pinned(v, *weights) for v in side1]
    far1 = from_far(*side1)
    middle = [(h, c, s, 1, v) for h, c, s, v in side_blocks(*side1)]
    weights = add_tiles(kinds(middle), slots, scales, where, weights, blocks(middle))
    late = [(h, c, s, 1, v) for h, c, s, v in far_blocks(*(pinned(v, *weights) for v in far1))]
    run = lambda rows, weight, parts, name: expert(
        kinds(late), slots, scales, where, rows, weight, weights, blocks(late), parts, name
    )
    plus_a, minus_a, plus_b, minus_b = run(sent, sent_weight, (128,) * 4, "expert_sent")
    got_a = shift(plus_a, "y", 1), shift(minus_a, "y", -1)
    got_b = shift(plus_b, "z", 1), shift(minus_b, "z", -1)
    rest = run(kept, kept_weight, (64, 64, 128) * 2, "expert_kept")
    out_a = ring_sum("y", "z", *got_a, *rest[:3])
    out_b = ring_sum("z", "y", *got_b, *rest[3:])
    return jnp.concatenate([out_a, out_b], axis=0).reshape(-1, hidden_rows.shape[1], D)


def solution(mesh):
    fine = Mesh(mesh.devices.reshape(4, 2, 4, 4), ("x", "c", "z", "y"))
    rows = ("x", "c")
    every = ("x", "c", "z", "y")
    return jax.shard_map(
        body,
        mesh=fine,
        in_specs=(
            P(rows, None, None),
            P(),
            P(rows, None, None),
            P(rows, None, None),
            P(EP, None, None),
            P(EP, None, None),
            P(EP, None, None),
            P(every, None, None),
            P(every),
            P(every, None),
            P(every),
        ),
        out_specs=P(every, None, None),
        check_vma=False,
    )
```
